256 devices in a mesh: seq: 64 (over x, y, z_lo), tensor: 4 (over z_hi, core).
Axes of the slice: x: 4, y: 4, z: 8 (z_hi: 2, z_lo: 4; z = z_hi * 4 + z_lo), core: 2. Of those that a mesh axis runs over, the one named last changes fastest.
Arguments:
- queries: bfloat16 [8192, 4096], P(('seq', 'tensor')), may hold values from -5 to 5
- keys: bfloat16 [8192, 1024], P(('seq', 'tensor')), may hold values from -5 to 5
- values: bfloat16 [8192, 1024], P(('seq', 'tensor')), may hold values from -5 to 5
- mamba_x: bfloat16 [8192, 8192], P(('seq', 'tensor')), may hold values from -5 to 5
- mamba_b: bfloat16 [8192, 1024], P(('seq', 'tensor')), may hold values from -5 to 5
- mamba_c: bfloat16 [8192, 1024], P(('seq', 'tensor')), may hold values from -5 to 5
- mamba_dt: bfloat16 [8192, 128], P(('seq', 'tensor')), may hold values from -4 to 4
- conv_x: bfloat16 [4, 8192], P(None, 'tensor'), may hold values from -3 to 3
- conv_b: bfloat16 [4, 1024], P(None, 'tensor'), may hold values from -3 to 3
- conv_c: bfloat16 [4, 1024], P(None, 'tensor'), may hold values from -3 to 3
- dt_bias: float32 [128], P('tensor'), may hold values from -1 to 1
- decay_rate: float32 [128], P('tensor'), may hold values from 0.0001 to 0.05
- skip_gain: float32 [128], P('tensor'), may hold values from 0.5 to 1.5
- norm_gain: float32 [8192], P('tensor'), may hold values from 0.5 to 1.5
- windows: int32 [32], replicated, may hold values from 1056 to 4224, as said below
- doc_lengths: int32 [3], replicated, may hold values from 1 to 6144, 8192 in all
Outputs:
- attn_out: bfloat16 [8192, 4096], P('seq', 'tensor')
- mamba_out: bfloat16 [8192, 8192], P('seq', 'tensor')
- attn_checksum: float32 [4096], P('tensor')
- mamba_checksum: float32 [8192], P('tensor')
The draws below stay inside these ranges and needn't reach their ends.
Inputs may be any that keep to these rules, and one draw needn't show every extreme that they name: `windows`: one of the 32 query heads has a window of exactly 4224 tokens. `doc_lengths`: 3 lengths summing to 8192; the longest is exactly three quarters of 8192.
All inputs are finite; a program needn't handle non-finite values.
Results may differ from the reference program's by a relative error of at most 0.007.
Values may be sent and summed in bfloat16 or wider, within the bound.
A program may use at most 192 MiB of HBM per device.

```python
import math
import jax
import jax.numpy as jnp
import numpy as np
from jax import lax

QUERY_HEAD_COUNT = 32
KEY_VALUE_HEADS = 8
HEAD_SIZE = 128
MH = 128
MP = 64
MN = 128
MG = 8
KC = 4
NDOC = 3
TOKENS_PER_INDEX = 128
SEQUENCE_LENGTH = 8192
LONGEST_WINDOW = 4224


def keys_common(key):
    starting_key = jax.random.fold_in(key, 101)
    unscaled_keys = jnp.clip(jax.random.normal(starting_key, (SEQUENCE_LENGTH, KEY_VALUE_HEADS * HEAD_SIZE), jnp.float32), -5.0, 5.0)
    return unscaled_keys


def draw_keys(key, part):
    return keys_common(key).astype(jnp.bfloat16)


def draw_queries(key, part):
    drawn_rows = jnp.clip(jax.random.normal(jax.random.fold_in(key, 202), (SEQUENCE_LENGTH, QUERY_HEAD_COUNT * HEAD_SIZE), jnp.float32), -5.0, 5.0)
    return drawn_rows.astype(jnp.bfloat16)


def draw_windows(key, part):
    widths = jax.random.randint(jax.random.fold_in(key, 303), (QUERY_HEAD_COUNT,), LONGEST_WINDOW // 4, LONGEST_WINDOW + 1)
    chosen = jax.random.randint(jax.random.fold_in(key, 304), (), 0, QUERY_HEAD_COUNT)
    return jnp.where(jnp.arange(QUERY_HEAD_COUNT) == chosen, LONGEST_WINDOW, widths).astype(jnp.int32)


def block_levels(own_key, shape, split, least, top_value):
    loudness = 1.0
    for axis_at, shards_of in split:
        steps = jax.random.uniform(jax.random.fold_in(jax.random.fold_in(own_key, 6), axis_at), (shards_of,), jnp.float32, least / len(split), top_value / len(split))
        loudness = loudness * jnp.repeat(jnp.exp(steps), shape[axis_at] // shards_of).reshape((-1,) + (1,) * (len(shape) - 1 - axis_at))
    return loudness


def profile(number_of, total, most, lean):
    loads = [(1 << 20) // math.isqrt(grade ** lean) + 1 for grade in range(2, number_of + 1)]
    spare, counts = total - most - (number_of - 1), [1] * (number_of - 1)
    while spare > 0:
        movable = [i for i in range(number_of - 1) if counts[i] < most]
        mass, left = sum([loads[i] for i in movable]), spare
        for i in movable:
            more = min(most - counts[i], max(1, left * loads[i] // mass), spare)
            counts[i] = counts[i] + more
            spare = spare - more
    return np.array([most] + counts)


def ragged_sizes(key, amount, total, most, skew):
    if amount == 2:
        one = jax.random.randint(key, (), max(1, total - most), min(most, total - 1) + 1)
        return jnp.stack([one, total - one])
    lengths = jnp.asarray(profile(amount, total, most, skew), jnp.int32)
    couples = (amount - 1) // 2
    giver, taker = lengths[1:1 + 2 * couples:2], lengths[2:2 + 2 * couples:2]
    slack = jnp.minimum(giver - 1, most - taker)
    shifted = jax.random.randint(jax.random.fold_in(key, 1), (couples,), 0, 1 << 20) % (slack + 1)
    lengths = lengths.at[1:1 + 2 * couples:2].set(giver - shifted).at[2:2 + 2 * couples:2].set(taker + shifted)
    return lengths[jax.random.permutation(jax.random.fold_in(key, 2), amount)]


def noise(own_key, shape, width, reach, cuts=(), kind=jnp.bfloat16):
    loudness = block_levels(own_key, shape, cuts, -0.22, 0.18) if cuts else 1.0
    result = jax.random.normal(own_key, shape, jnp.float32) * width * loudness
    return jnp.minimum(jnp.maximum(result, -reach), reach).astype(kind)


def setup_inputs(seed: int = 0) -> dict:
    splits = jax.random.split(jax.random.key(seed), 17)
    return {
        "queries": draw_queries(jax.random.fold_in(splits[16], 71), 0),
        "keys": draw_keys(jax.random.fold_in(splits[16], 71), 0),
        "values": noise(splits[2], (SEQUENCE_LENGTH, KEY_VALUE_HEADS * HEAD_SIZE), 1.0, 5.0, ((0, 256),)),
        "mamba_x": noise(splits[3], (SEQUENCE_LENGTH, MH * MP), 1.0, 5.0, ((0, 256),)),
        "mamba_b": noise(splits[4], (SEQUENCE_LENGTH, MG * MN), 1.0, 5.0, ((0, 256),)),
        "mamba_c": noise(splits[5], (SEQUENCE_LENGTH, MG * MN), 1.0, 5.0, ((0, 256),)),
        "mamba_dt": noise(splits[6], (SEQUENCE_LENGTH, MH), 1.0, 4.0, ((0, 256),)),
        "conv_x": noise(splits[7], (KC, MH * MP), KC ** -0.5, 3.0, ((1, 4),)),
        "conv_b": noise(splits[8], (KC, MG * MN), KC ** -0.5, 3.0, ((1, 4),)),
        "conv_c": noise(splits[9], (KC, MG * MN), KC ** -0.5, 3.0, ((1, 4),)),
        "dt_bias": jnp.clip(jax.random.uniform(splits[10], (MH,), jnp.float32, -1.0, 1.0) * block_levels(splits[10], (MH,), ((0, 4),), -0.4, 0.0), -1.0, 1.0),
        "decay_rate": jnp.clip(jnp.exp(math.log(0.05) - 6.214608 * jax.random.uniform(splits[11], (MH,), jnp.float32) ** block_levels(splits[11], (MH,), ((0, 4),), -0.2, 0.2)), 0.0001, 0.05),
        "skip_gain": jnp.clip(0.5 + 1.0 * jax.random.uniform(splits[12], (MH,), jnp.float32) ** block_levels(splits[12], (MH,), ((0, 4),), -0.2, 0.2), 0.5, 1.5),
        "norm_gain": jnp.clip(1.0 + 0.1 * jax.random.normal(splits[13], (MH * MP,), jnp.float32), 0.5, 1.5),
        "windows": draw_windows(jax.random.fold_in(splits[16], 71), 0),
        "doc_lengths": ragged_sizes(splits[15], NDOC, SEQUENCE_LENGTH, 3 * SEQUENCE_LENGTH // 4, 1).astype(jnp.int32),
    }


NEG_LARGE = -1e+30
EPS_NORM = 1e-05

def doc_table(doc_lengths):
    return (jnp.cumsum(doc_lengths) - doc_lengths).astype(jnp.int32)

def doc_index(positions, doc_starts):
    return lax.optimization_barrier(jnp.sum((positions[:, None] >= doc_starts[None, :]).astype(jnp.int32), axis=1)) - 1

def allowed_mask(query_pos, key_pos, doc_starts, window_per_head):
    gap = query_pos[:, None] - key_pos[None, :]
    same_doc = doc_index(query_pos, doc_starts)[:, None] == doc_index(key_pos, doc_starts)[None, :]
    base_ok = (gap >= 0) & (key_pos[None, :] >= 0) & same_doc
    return base_ok[None, None] & (gap[None, None] < window_per_head[:, :, None, None])

def reference_attention(queries, keys, values, windows, doc_starts):
    group_width = QUERY_HEAD_COUNT // KEY_VALUE_HEADS
    window_per_head = windows.reshape(KEY_VALUE_HEADS, group_width)
    block_count = SEQUENCE_LENGTH // TOKENS_PER_INDEX
    padded_keys = jnp.pad(keys, ((LONGEST_WINDOW, 0), (0, 0)))
    padded_values = jnp.pad(values, ((LONGEST_WINDOW, 0), (0, 0)))

    def one_block(index):
        first = (index * TOKENS_PER_INDEX).astype(jnp.int32)
        query_tile_block = lax.dynamic_slice_in_dim(queries, first, TOKENS_PER_INDEX, 0)
        key_tile_block = lax.dynamic_slice_in_dim(padded_keys, first, LONGEST_WINDOW + TOKENS_PER_INDEX, 0)
        value_tile_block = lax.dynamic_slice_in_dim(padded_values, first, LONGEST_WINDOW + TOKENS_PER_INDEX, 0)
        query_pos = first + jnp.arange(TOKENS_PER_INDEX, dtype=jnp.int32)
        key_pos = first - LONGEST_WINDOW + jnp.arange(LONGEST_WINDOW + TOKENS_PER_INDEX, dtype=jnp.int32)
        grouped_heads = query_tile_block.reshape(TOKENS_PER_INDEX, KEY_VALUE_HEADS, group_width, HEAD_SIZE).astype(jnp.float32)
        keys_rank3 = key_tile_block.reshape(LONGEST_WINDOW + TOKENS_PER_INDEX, KEY_VALUE_HEADS, HEAD_SIZE).astype(jnp.float32)
        values_rank3 = value_tile_block.reshape(LONGEST_WINDOW + TOKENS_PER_INDEX, KEY_VALUE_HEADS, HEAD_SIZE).astype(jnp.float32)
        scores = jnp.einsum('tgqd,sgd->gqts', grouped_heads, keys_rank3) * (1.0 / math.sqrt(HEAD_SIZE))
        allowed = allowed_mask(query_pos, key_pos, doc_starts, window_per_head)
        scores = jnp.where(allowed, scores, NEG_LARGE)
        top_score = lax.optimization_barrier(jnp.max(scores, axis=-1, keepdims=True))
        weights = jnp.where(allowed, jnp.exp(scores - top_score), 0.0)
        totals = lax.optimization_barrier(jnp.sum(weights, axis=-1))
        rounded = weights.astype(jnp.bfloat16).astype(jnp.float32)
        mixed = jnp.einsum('gqts,sgd->gqtd', rounded, values_rank3)
        output = mixed / totals[..., None]
        return output.transpose(2, 0, 1, 3).reshape(TOKENS_PER_INDEX, QUERY_HEAD_COUNT * HEAD_SIZE).astype(jnp.bfloat16)
    blocks = lax.map(one_block, jnp.arange(block_count, dtype=jnp.int32))
    return blocks.reshape(SEQUENCE_LENGTH, QUERY_HEAD_COUNT * HEAD_SIZE)

def causal_conv(extended, taps, positions, doc_starts):
    count = positions.shape[0]
    docs_out = doc_index(positions, doc_starts)
    ext_pos = positions[0] - (KC - 1) + jnp.arange(count + KC - 1, dtype=jnp.int32)
    docs_ext = doc_index(ext_pos, doc_starts)
    running = jnp.zeros((count, extended.shape[1]), jnp.float32)
    for tap_index in range(KC):
        offset = KC - 1 - tap_index
        valid = (docs_ext[offset:offset + count] == docs_out) & (ext_pos[offset:offset + count] >= 0)
        term = taps[tap_index].astype(jnp.float32)[None, :] * extended[offset:offset + count].astype(jnp.float32)
        running = running + jnp.where(valid[:, None], term, 0.0)
    return jax.nn.silu(running).astype(jnp.bfloat16)

def stretch_terms(x_rows, b_rows, c_rows, dt_rows, positions, doc_starts, dt_bias, decay_rate):
    count = positions.shape[0]
    heads = x_rows.shape[1] // MP
    groups = b_rows.shape[1] // MN
    per_group = heads // groups
    docs = doc_index(positions, doc_starts)
    prior_doc = doc_index(positions[:1] - 1, doc_starts)[0]
    delta = jax.nn.softplus(dt_rows.astype(jnp.float32) + dt_bias[None, :])
    log_decay = -delta * decay_rate[None, :]
    running = jnp.cumsum(log_decay, axis=0)
    running_heads = running.T
    order = jnp.arange(count, dtype=jnp.int32)
    causal = order[:, None] >= order[None, :]
    same_doc = docs[:, None] == docs[None, :]
    gaps = running_heads[:, :, None] - running_heads[:, None, :]
    segment = jnp.where((causal & same_doc)[None], jnp.exp(jnp.minimum(gaps, 0.0)), 0.0)
    inputs3 = x_rows.reshape(count, heads, MP)
    b_groups = b_rows.reshape(count, groups, MN)
    c_groups = c_rows.reshape(count, groups, MN)
    cross = jnp.einsum('tgn,sgn->gts', c_groups.astype(jnp.float32), b_groups.astype(jnp.float32))
    cross_heads = jnp.repeat(cross, per_group, axis=0)
    mixing = (segment * cross_heads * delta.T[:, None, :]).astype(jnp.bfloat16)
    intra = jnp.einsum('hts,shp->thp', mixing.astype(jnp.float32), inputs3.astype(jnp.float32))
    last_doc = docs[count - 1]
    to_end = jnp.where((docs == last_doc)[:, None], jnp.exp(running[count - 1][None, :] - running), 0.0) * delta
    weighted = (inputs3.astype(jnp.float32) * to_end[:, :, None]).astype(jnp.bfloat16)
    b_heads = jnp.repeat(b_groups, per_group, axis=1)
    local_state = jnp.einsum('shp,shn->hpn', weighted.astype(jnp.float32), b_heads.astype(jnp.float32))
    carry_factor = jnp.where(prior_doc == last_doc, jnp.exp(running[count - 1]), 0.0)
    inflow = jnp.where((docs == prior_doc)[:, None], jnp.exp(running), 0.0)
    c_heads = jnp.repeat(c_groups, per_group, axis=1)
    return (intra, local_state, carry_factor, inflow, c_heads)

def stretch_finish(intra, incoming, inflow, c_heads, x_rows, skip_gain, norm_gain):
    count = x_rows.shape[0]
    heads = x_rows.shape[1] // MP
    incoming_bf = incoming.astype(jnp.bfloat16)
    entering = jnp.einsum('thn,hpn->thp', c_heads.astype(jnp.float32), incoming_bf.astype(jnp.float32)) * inflow[:, :, None]
    inputs3 = x_rows.reshape(count, heads, MP).astype(jnp.float32)
    mixed = intra + entering + skip_gain[None, :, None] * inputs3
    mean_square = lax.optimization_barrier(jnp.mean(mixed * mixed, axis=-1, keepdims=True))
    normed = mixed * lax.rsqrt(mean_square + EPS_NORM) * norm_gain.reshape(heads, MP)[None]
    return normed.reshape(count, heads * MP).astype(jnp.bfloat16)

def reference(queries, keys, values, mamba_x, mamba_b, mamba_c, mamba_dt, conv_x, conv_b, conv_c, dt_bias, decay_rate, skip_gain, norm_gain, windows, doc_lengths):
    doc_starts = doc_table(doc_lengths)
    attention = reference_attention(queries, keys, values, windows, doc_starts)
    positions = jnp.arange(SEQUENCE_LENGTH, dtype=jnp.int32)
    pad_rows = ((KC - 1, 0), (0, 0))
    conv_x_out = causal_conv(jnp.pad(mamba_x, pad_rows), conv_x, positions, doc_starts)
    conv_b_out = causal_conv(jnp.pad(mamba_b, pad_rows), conv_b, positions, doc_starts)
    conv_c_out = causal_conv(jnp.pad(mamba_c, pad_rows), conv_c, positions, doc_starts)
    stretch_count = SEQUENCE_LENGTH // TOKENS_PER_INDEX

    def stretch_step(incoming, inputs):
        index, x_rows, b_rows, c_rows, dt_rows = inputs
        stretch_pos = index * TOKENS_PER_INDEX + jnp.arange(TOKENS_PER_INDEX, dtype=jnp.int32)
        intra, local_state, carry_factor, inflow, c_heads = stretch_terms(x_rows, b_rows, c_rows, dt_rows, stretch_pos, doc_starts, dt_bias, decay_rate)
        output = stretch_finish(intra, incoming, inflow, c_heads, x_rows, skip_gain, norm_gain)
        updated = carry_factor[:, None, None] * incoming + local_state
        return (updated, output)
    initial = jnp.zeros((MH, MP, MN), jnp.float32)
    scanned = (jnp.arange(stretch_count, dtype=jnp.int32), conv_x_out.reshape(stretch_count, TOKENS_PER_INDEX, MH * MP), conv_b_out.reshape(stretch_count, TOKENS_PER_INDEX, MG * MN), conv_c_out.reshape(stretch_count, TOKENS_PER_INDEX, MG * MN), mamba_dt.reshape(stretch_count, TOKENS_PER_INDEX, MH))
    final_state, outputs = lax.scan(stretch_step, initial, scanned)
    mamba_out = outputs.reshape(SEQUENCE_LENGTH, MH * MP)
    return (attention, mamba_out, lax.optimization_barrier(jnp.sum(attention.astype(jnp.float32), axis=0)), lax.optimization_barrier(jnp.sum(mamba_out.astype(jnp.float32), axis=0)))
```

```python
import math

import jax
import jax.numpy as jnp
from jax import lax
from jax.experimental import pallas as pl
from jax.experimental.pallas import tpu as pltpu
from jax.sharding import Mesh
from jax.sharding import PartitionSpec as P

AXES = ("X", "Y", "zl", "zh", "c")
MESH_ID = pl.DeviceIdType.MESH
BF = jnp.bfloat16
F32 = jnp.float32
HIGH = lax.Precision.HIGHEST
NEG_LARGE = -1e30
EPS_NORM = 1e-05
SUPER = 512
KV_ROWS = 5120
BACK = 4352
VM = pl.BlockSpec(memory_space=pltpu.VMEM)
SM = pl.BlockSpec(memory_space=pltpu.SMEM)
NT = (((1,), (1,)), ((), ()))
TN = (((0,), (0,)), ((), ()))


def coords():
    return tuple(lax.axis_index(a) for a in AXES)


def aligned(v, n):
    return pl.multiple_of(v, n)


def landed(dst, sem):
    pltpu.make_async_copy(dst, dst, sem).wait()


def exchange_in(
    q, k, v, x, b, c, dt,
    qo, kvo, xo, bo, co, dto, txo, tbo, tco,
    sq, rq, sx, rx, st, rt, sg, rg, sf, rf,
):
    X, Y, Z, H, C = coords()
    s = X * 4 + Y
    T = H * 2 + C
    u = Z * 4 + T
    zz = H * 4 + Z
    half = lax.div(Z, 2)
    bar = pltpu.get_barrier_semaphore()

    def signal(**where):
        pl.semaphore_signal(bar, 1, device_id=where, device_id_type=MESH_ID)

    def at(super_index):
        n = lax.rem(super_index + 16, 16)
        return {"X": lax.div(n, 4), "Y": lax.rem(n, 4)}

    def chip(o):
        n = lax.rem(zz + o, 8)
        return lax.div(n, 4), lax.rem(n, 4)

    others = [(o, e) for o in (1, 7, 2, 6, 3, 5, 4) for e in (0, 1)] + [(0, 1)]
    for o, e in others:
        zh, zl = chip(o)
        signal(zl=zl, zh=zh, c=lax.rem(C + e, 2))
    for d in range(1, 9):
        @pl.when(s >= d)
        def _():
            signal(**at(s - d))
    @pl.when(jnp.logical_and(C == 0, s >= 9))
    def _():
        signal(**at(s - 9), c=1)
    signal(**at(s - 1), zl=3, zh=1, c=1)

    kvo[0:128, :] = jnp.zeros((128, 256), BF)
    kvo[4864:5120, :] = jnp.zeros((256, 256), BF)

    expected = 15 + jnp.minimum(8, 15 - s)
    expected += jnp.where(jnp.logical_and(C == 1, s <= 6), 1, 0)
    expected += jnp.where(u == 15, 16, 0)
    pl.semaphore_wait(bar, expected)

    srow = lax.rem(Z, 2) * 128 + T * 32
    slot = lax.rem(Z, 2) * 4 + T

    def qkv_parts(o):
        zh, zl = chip(o)
        g = zh * 4 + zl
        krow = BACK + half * 256 + srow
        k_dst = kvo.at[pl.ds(aligned(krow, 32), 32), 0:128]
        v_dst = kvo.at[pl.ds(aligned(krow, 32), 32), 128:256]
        q_dst = qo.at[pl.ds(aligned(srow, 32), 32), :]
        k_src = k.at[:, pl.ds(aligned(g * 128, 128), 128)]
        v_src = v.at[:, pl.ds(aligned(g * 128, 128), 128)]
        q_src = q.at[:, pl.ds(aligned(g * 512, 512), 512)]
        return {"zh": zh, "zl": zl, "c": half}, ((k_src, k_dst), (v_src, v_dst), (q_src, q_dst))

    def qkv_copy(o, i):
        where, parts = qkv_parts(o)
        src, dst = parts[i]
        return pltpu.make_async_remote_copy(
            src, dst, sq.at[i, o], rq.at[i, slot], device_id=where, device_id_type=MESH_ID
        )

    order8 = (4, 3, 5, 2, 6, 1, 7)
    for o in order8:
        qkv_copy(o, 0).start()
        qkv_copy(o, 1).start()

    @pl.when(half != C)
    def _():
        qkv_copy(0, 0).start()
        qkv_copy(0, 1).start()

    @pl.when(half == C)
    def _():
        for src, dst in qkv_parts(0)[1]:
            dst[...] = src[...]

    def col_parts(o, e):
        zh, zl = chip(o)
        cc = lax.rem(C + e, 2)
        tensor = zh * 2 + cc
        xcol = tensor * 2048 + zl * 512
        gcol = (tensor * 2 + lax.div(zl, 2)) * 128
        rows = pl.ds(aligned(u * 32, 32), 32)
        wide = pl.ds(aligned(xcol, 512), 512)
        thin = pl.ds(aligned(gcol, 128), 128)
        return {"zh": zh, "zl": zl, "c": cc}, (
            (dt, dto.at[rows, :]),
            (b.at[:, thin], bo.at[rows, :]),
            (c.at[:, thin], co.at[rows, :]),
            (x.at[:, wide], xo.at[rows, :]),
        )

    def col_copy(o, e, i):
        where, parts = col_parts(o, e)
        src, dst = parts[i]
        return pltpu.make_async_remote_copy(
            src, dst, sx.at[i, o * 2 + e], rx.at[i, u], device_id=where, device_id_type=MESH_ID
        )

    order16 = [(o, e) for o in order8 for e in (0, 1)] + [(0, 1)]
    for i in range(3):
        for o, e in order16:
            col_copy(o, e, i).start()

    def tail_copy(o, e, i):
        zh, zl = chip(o)
        cc = lax.rem(C + e, 2)
        tensor = zh * 2 + cc
        xcol = tensor * 2048 + zl * 512
        gcol = (tensor * 2 + lax.div(zl, 2)) * 128
        src, dst, col, wide = ((x, txo, xcol, 512), (b, tbo, gcol, 128), (c, tco, gcol, 128))[i]
        return pltpu.make_async_remote_copy(
            src.at[16:32, pl.ds(aligned(col, wide), wide)], dst,
            st.at[i, o * 2 + e], rt.at[i],
            device_id={**at(s + 1), "zh": zh, "zl": zl, "c": cc}, device_id_type=MESH_ID,
        )

    for o, e in order16:
        col_copy(o, e, 3).start()
    for i, (src, dst) in enumerate(col_parts(0, 0)[1]):
        dst[...] = src[...]

    @pl.when(u == 15)
    def _():
        for o in range(8):
            for e in (0, 1):
                for i in range(3):
                    tail_copy(o, e, i).start()

    for o in order8:
        qkv_copy(o, 2).start()

    @pl.when(half != C)
    def _():
        qkv_copy(0, 2).start()

    def qkv_landed(i):
        for j in range(2):
            for t in range(4):
                row = j * 128 + t * 32
                if i == 2:
                    dst = qo.at[row:row + 32, :]
                else:
                    krow = aligned(BACK + C * 256 + row, 32)
                    dst = kvo.at[pl.ds(krow, 32), i * 128:i * 128 + 128]

                @pl.when(jnp.logical_or(2 * C + j != Z, T != t))
                def _():
                    landed(dst, rq.at[i, j * 4 + t])

    qkv_landed(0)
    qkv_landed(1)

    def half_rows(d):
        return kvo.at[pl.ds(aligned(BACK - SUPER * d + C * 256, 256), 256), :]

    def partner_rows(d):
        return kvo.at[pl.ds(aligned(BACK - SUPER * d + (1 - C) * 256, 256), 256), :]

    def pass_on(d):
        return pltpu.make_async_remote_copy(
            half_rows(0), half_rows(d), sg.at[d], rg.at[d], device_id=at(s + d), device_id_type=MESH_ID
        )

    def pass_last():
        return pltpu.make_async_remote_copy(
            kvo.at[BACK + 384:BACK + 512, :], kvo.at[128:256, :], sg.at[9], rg.at[9],
            device_id={**at(s + 9), "c": 0}, device_id_type=MESH_ID,
        )

    def to_partner(d):
        return pltpu.make_async_remote_copy(
            half_rows(d), half_rows(d), sf.at[d], rf.at[d], device_id={"c": 1 - C}, device_id_type=MESH_ID
        )

    last_out = jnp.logical_and(C == 1, s <= 6)
    for d in range(1, 9):
        @pl.when(s + d < 16)
        def _():
            pass_on(d).start()

    @pl.when(last_out)
    def _():
        pass_last().start()

    to_partner(0).start()
    for d in range(1, 9):
        @pl.when(s >= d)
        def _():
            landed(half_rows(d), rg.at[d])
            to_partner(d).start()

    for i in range(4):
        for o, e in order16:
            zs = lax.rem(zz + 8 - o, 8)
            us = lax.rem(zs, 4) * 4 + lax.div(zs, 4) * 2 + lax.rem(C + e, 2)
            dst = (dto, bo, co, xo)[i].at[pl.ds(aligned(us * 32, 32), 32), :]
            landed(dst, rx.at[i, us])
    for i in range(3):
        landed((txo, tbo, tco)[i], rt.at[i])
    qkv_landed(2)

    @pl.when(jnp.logical_and(C == 0, s >= 9))
    def _():
        landed(kvo.at[128:256, :], rg.at[9])

    landed(partner_rows(0), rf.at[0])
    for d in range(1, 9):
        @pl.when(s >= d)
        def _():
            landed(partner_rows(d), rf.at[d])

    for i in range(3):
        for o in order8:
            qkv_copy(o, i).wait_send()

        @pl.when(half != C)
        def _():
            qkv_copy(0, i).wait_send()
    for i in range(4):
        for o, e in order16:
            col_copy(o, e, i).wait_send()

    @pl.when(u == 15)
    def _():
        for o in range(8):
            for e in (0, 1):
                for i in range(3):
                    tail_copy(o, e, i).wait_send()
    to_partner(0).wait_send()
    for d in range(1, 9):
        @pl.when(s + d < 16)
        def _():
            pass_on(d).wait_send()

        @pl.when(s >= d)
        def _():
            to_partner(d).wait_send()

    @pl.when(last_out)
    def _():
        pass_last().wait_send()


def call_exchange_in(arrays):
    shapes = ((256, 512), (KV_ROWS, 256), (512, 512), (512, 128), (512, 128), (512, 128),
              (16, 512), (16, 128), (16, 128))
    dma = pltpu.SemaphoreType.DMA
    return pl.pallas_call(
        exchange_in,
        out_shape=[jax.ShapeDtypeStruct(n, BF) for n in shapes],
        in_specs=[VM] * 7,
        out_specs=[VM] * 9,
        scratch_shapes=[
            dma((3, 8)), dma((3, 8)), dma((4, 16)), dma((4, 16)), dma((3, 16)), dma((3,)),
            dma((10,)), dma((10,)), dma((9,)), dma((9,)),
        ],
        compiler_params=pltpu.CompilerParams(collective_id=1, has_side_effects=True),
        name="exchange_in",
    )(*arrays)


def spread_matrix(rows, cols):
    a = lax.broadcasted_iota(jnp.int32, (rows, cols), 0)
    b = lax.broadcasted_iota(jnp.int32, (rows, cols), 1)
    if rows < cols:
        return (lax.div(b, 64) == a).astype(F32)
    return (lax.div(a, 64) == b).astype(F32)


def dot(a, b, dims=(((1,), (0,)), ((), ())), precision=None):
    return lax.dot_general(a, b, dims, precision=precision, preferred_element_type=F32)


def doc_of(pos, s1, s2):
    one = jnp.where(pos >= s1, 1, 0) + jnp.where(pos >= s2, 1, 0)
    return jnp.where(pos >= 0, one, -1)


def softplus(z):
    return jnp.maximum(z, 0.0) + jnp.log1p(jnp.exp(-jnp.abs(z)))


def mamba_local(
    lens, x, b, c, dt, tx, tb, tc, conv_x, conv_b, conv_c, bias, rate, skip,
    base_o, inflow_o, cc_o, part_o, decay_o, send_o,
    xs, bs, cs,
):
    X, Y, Z, H, C = coords()
    s = X * 4 + Y
    T = H * 2 + C
    s1 = lens[0]
    s2 = lens[0] + lens[1]
    p0 = s * SUPER
    lane8 = lax.broadcasted_iota(jnp.int32, (8, 32), 1)
    sub8 = lax.broadcasted_iota(jnp.int32, (8, 32), 0)
    own = lane8 == sub8 + 8 * Z

    def column(ref):
        return jnp.sum(jnp.where(own, ref[...], 0.0), axis=1, keepdims=True)

    pick32 = (lax.broadcasted_iota(jnp.int32, (32, 8), 0)
              == lax.broadcasted_iota(jnp.int32, (32, 8), 1) + 8 * Z).astype(F32)

    def row(ref):
        return dot(ref[...], pick32, precision=HIGH)

    first_head = T * 32 + Z * 8
    pick = (lax.broadcasted_iota(jnp.int32, (128, 8), 0)
            == lax.broadcasted_iota(jnp.int32, (128, 8), 1) + first_head).astype(BF)
    dcol = softplus(dot(dt[...], pick) + row(bias))
    drow = softplus(dot(pick, dt[...], (((0,), (1,)), ((), ()))) + column(bias))
    lcol = -dcol * row(rate)
    lrow = -drow * column(rate)
    wide = spread_matrix(8, 512)
    tall = spread_matrix(512, 8)
    skip_wide = dot(row(skip), wide, precision=HIGH)

    for src, tail, buf in ((x, tx, xs), (b, tb, bs), (c, tc, cs)):
        buf[0:16, :] = tail[...].astype(F32)
        buf[16:528, :] = src[...].astype(F32)
    taps_x = conv_x[:, pl.ds(aligned(Z * 512, 512), 512)].astype(F32)
    group = pl.ds(aligned(lax.div(Z, 2) * 128, 128), 128)
    taps_b = conv_b[:, group].astype(F32)
    taps_c = conv_c[:, group].astype(F32)

    ti = lax.broadcasted_iota(jnp.int32, (128, 128), 0)
    si = lax.broadcasted_iota(jnp.int32, (128, 128), 1)
    lower = (ti >= si).astype(F32)
    upper = (ti <= si).astype(F32)
    lane = lax.broadcasted_iota(jnp.int32, (128, 128), 1)
    state = jnp.zeros((512, 128), F32)
    decay = jnp.ones((8, 128), F32)
    for n in range(4):
        pb = p0 + n * 128
        rows = slice(n * 128, n * 128 + 128)
        pcol = pb + lax.broadcasted_iota(jnp.int32, (128, 1), 0)
        prow = pb + lax.broadcasted_iota(jnp.int32, (1, 128), 1)
        start = jnp.where(pcol >= s2, s2, jnp.where(pcol >= s1, s1, 0))
        keep = [pcol - j >= start for j in range(4)]

        def conv(buf, taps):
            total = None
            for j in range(4):
                lo = 16 + n * 128 - j
                term = taps[j:j + 1, :] * buf[lo:lo + 128, :]
                if j:
                    term = jnp.where(keep[j], term, 0.0)
                total = term if total is None else total + term
            return (total / (1.0 + jnp.exp(-total))).astype(BF)

        xc = conv(xs, taps_x)
        bc = conv(bs, taps_b)
        cc = conv(cs, taps_c)
        cc_o[rows, :] = cc
        ccol = dot(lower, lcol[rows, :], precision=HIGH)
        crow = dot(lrow[:, rows], upper, precision=HIGH)
        dcol_n = dcol[rows, :]
        drow_n = drow[:, rows]
        doc_c = doc_of(pcol, s1, s2)
        doc_r = doc_of(prow, s1, s2)
        allowed = jnp.logical_and(ti >= si, doc_c == doc_r)
        cross = jnp.where(allowed, dot(cc, bc, NT), 0.0)
        xf = xc.astype(F32)
        for pair in range(4):
            mixes = []
            for h in (2 * pair, 2 * pair + 1):
                gap = ccol[:, h:h + 1] - crow[h:h + 1, :]
                seg = jnp.exp(jnp.minimum(gap, 0.0))
                mixes.append((seg * cross * drow_n[h:h + 1, :]).astype(BF))
            xp = xc[:, pair * 128:pair * 128 + 128]
            zero = jnp.zeros_like(xp)
            both = jnp.concatenate(
                [jnp.where(lane < 64, xp, zero), jnp.where(lane < 64, zero, xp)], axis=0)
            intra = dot(jnp.concatenate(mixes, axis=1), both)
            cols = slice(pair * 128, pair * 128 + 128)
            base_o[rows, cols] = intra + skip_wide[:, cols] * xf[:, cols]
        pe = pb + 127
        doc_e = doc_of(pe, s1, s2)
        doc_p = doc_of(pb - 1, s1, s2)
        to_end = jnp.where(doc_c == doc_e, jnp.exp(ccol[127:128, :] - ccol), 0.0) * dcol_n
        weighted = (dot(to_end, wide, precision=HIGH) * xf).astype(BF)
        local = dot(weighted, bc, TN)
        factor = jnp.where(doc_p == doc_e, jnp.exp(crow[:, 127:128]), 0.0)
        factor = jnp.broadcast_to(factor, (8, 128))
        inflow_o[rows, :] = jnp.where(doc_c == doc_p, jnp.exp(ccol), 0.0)
        state = dot(tall, factor, precision=HIGH) * state + local
        decay = factor * decay
        if n < 3:
            part_o[n] = state
            decay_o[n] = decay
    for j in range(16):
        send_o[j, 0:32, :] = state[j * 32:j * 32 + 32, :]
        send_o[j, 32:40, :] = jnp.broadcast_to(decay[j // 2:j // 2 + 1, :], (8, 128))


def call_mamba_local(*args):
    out = [((512, 512), F32), ((512, 8), F32), ((512, 128), BF), ((3, 512, 128), F32),
           ((3, 8, 128), F32), ((16, 40, 128), F32)]
    return pl.pallas_call(
        mamba_local,
        out_shape=[jax.ShapeDtypeStruct(n, t) for n, t in out],
        in_specs=[SM] + [VM] * 13,
        out_specs=[VM] * 6,
        scratch_shapes=[pltpu.VMEM((528, 512), F32), pltpu.VMEM((528, 128), F32),
                        pltpu.VMEM((528, 128), F32)],
        name="mamba_local",
    )(*args)


def pass_states(send, inc, got, back, s1, r1, s2, r2):
    X, Y, Z, H, C = coords()
    s = X * 4 + Y
    bar = pltpu.get_barrier_semaphore()

    def peer(d):
        n = lax.rem(s + d, 16)
        return n, {"X": lax.div(n, 4), "Y": lax.rem(n, 4)}

    for d in range(1, 16):
        pl.semaphore_signal(bar, 1, device_id=peer(d)[1], device_id_type=MESH_ID)
    pl.semaphore_wait(bar, 15)

    def there(d):
        n, where = peer(d)
        return pltpu.make_async_remote_copy(
            send.at[n], got.at[s], s1.at[d], r1.at[s], device_id=where, device_id_type=MESH_ID)

    def again(d):
        n, where = peer(d)
        rows = pl.ds(aligned(s * 32, 32), 32)
        return pltpu.make_async_remote_copy(
            back.at[n], inc.at[rows, :], s2.at[d], r2.at[s], device_id=where, device_id_type=MESH_ID)

    for d in range(1, 16):
        there(d).start()
    got[s] = send[s]
    for d in range(1, 16):
        n, _ = peer(16 - d)
        landed(got.at[n], r1.at[n])
    value = jnp.zeros((4, 8, 128), F32)
    for n in range(16):
        back[n] = value.reshape(32, 128).astype(BF)
        value = got[n, 32:40, :][None] * value + got[n, 0:32, :].reshape(4, 8, 128)
    for d in range(1, 16):
        again(d).start()
    inc[pl.ds(aligned(s * 32, 32), 32), :] = back[s]
    for d in range(1, 16):
        n, _ = peer(16 - d)
        landed(inc.at[pl.ds(aligned(n * 32, 32), 32), :], r2.at[n])
    for d in range(1, 16):
        there(d).wait_send()
        again(d).wait_send()


def call_pass_states(send):
    dma = pltpu.SemaphoreType.DMA
    return pl.pallas_call(
        pass_states,
        out_shape=jax.ShapeDtypeStruct((512, 128), BF),
        in_specs=[VM],
        out_specs=VM,
        scratch_shapes=[pltpu.VMEM((16, 40, 128), F32), pltpu.VMEM((16, 32, 128), BF),
                        dma((16,)), dma((16,)), dma((16,)), dma((16,))],
        compiler_params=pltpu.CompilerParams(collective_id=2, has_side_effects=True),
        name="pass_states",
    )(send)


def mamba_finish(base, inflow, cc, part, decay, inc, gain, out, sums):
    Z = lax.axis_index("zl")
    wide = spread_matrix(8, 512)
    tall = spread_matrix(512, 8)
    gain_row = gain[:, pl.ds(aligned(Z * 512, 512), 512)]
    a = lax.broadcasted_iota(jnp.int32, (128, 128), 0)
    b = lax.broadcasted_iota(jnp.int32, (128, 128), 1)
    average = jnp.where(lax.div(a, 64) == lax.div(b, 64), 1.0 / 64, 0.0).astype(F32)
    entering = inc[...].astype(F32)
    total = jnp.zeros((1, 512), F32)
    for n in range(4):
        rows = slice(n * 128, n * 128 + 128)
        if n == 0:
            state = inc[...]
        else:
            state = (dot(tall, decay[n - 1], precision=HIGH) * entering + part[n - 1]).astype(BF)
        flow = dot(inflow[rows, :], wide, precision=HIGH)
        full = base[rows, :] + dot(cc[rows, :], state, NT) * flow
        for pair in range(4):
            cols = slice(pair * 128, pair * 128 + 128)
            f = full[:, cols]
            mean = dot(f * f, average, precision=HIGH)
            out[rows, cols] = (f * lax.rsqrt(mean + EPS_NORM) * gain_row[:, cols]).astype(BF)
        total = total + jnp.sum(out[rows, :].astype(F32), axis=0, keepdims=True)
    for i in range(4):
        sums[i:i + 1, :] = total[:, i * 128:i * 128 + 128]
    sums[4:8, :] = jnp.zeros((4, 128), F32)


def call_mamba_finish(*args):
    return pl.pallas_call(
        mamba_finish,
        out_shape=[jax.ShapeDtypeStruct((512, 512), BF), jax.ShapeDtypeStruct((8, 128), F32)],
        in_specs=[VM] * 7,
        out_specs=[VM] * 2,
        name="mamba_finish",
    )(*args)


def attend(windows, lens, q, kv, msum, out, sums, scores, top, acc, tot):
    X, Y, Z, H, C = coords()
    s = X * 4 + Y
    t0 = s * SUPER + C * 256
    base = s * SUPER - BACK
    s1 = lens[0]
    s2 = lens[0] + lens[1]
    scale = math.log2(math.e) / math.sqrt(128)

    def doc_start(t):
        return jnp.where(t >= s2, s2, jnp.where(t >= s1, s1, 0))

    tcol = t0 + lax.broadcasted_iota(jnp.int32, (256, 1), 0)
    start_col = doc_start(tcol)
    lane = lax.broadcasted_iota(jnp.int32, (1, 512), 1)
    end_row = BACK + C * 256 + 256
    sums[0:4, :] = msum[0:4, :]
    for h in range(4):
        w = windows[(H * 4 + Z) * 4 + h]
        low = jnp.maximum(tcol - w + 1, start_col)
        low_first = jnp.maximum(t0 - w + 1, doc_start(t0))
        c0 = lax.div(low_first - base, 256)
        count = lax.div(end_row - c0 * 256 + 511, 512)
        qh = q[:, h * 128:h * 128 + 128]
        top[...] = jnp.full((256, 128), NEG_LARGE, F32)
        acc[...] = jnp.zeros((256, 128), F32)
        tot[...] = jnp.zeros((256, 128), F32)

        @pl.loop(0, count)
        def _(i):
            r = aligned(c0 * 256 + i * 512, 256)
            score = dot(qh, kv[pl.ds(r, 512), 0:128], NT)
            kpos = base + r + lane
            ok = jnp.logical_and(kpos >= low, kpos <= tcol)
            score = jnp.where(ok, score, NEG_LARGE)
            scores[:, pl.ds(aligned(i * 512, 512), 512)] = score
            best = jnp.maximum(jnp.maximum(score[:, 0:128], score[:, 128:256]),
                               jnp.maximum(score[:, 256:384], score[:, 384:512]))
            top[...] = jnp.maximum(top[...], best)

        best = jnp.max(top[...], axis=1, keepdims=True)

        @pl.loop(0, count)
        def _(i):
            r = aligned(c0 * 256 + i * 512, 256)
            weight = jnp.exp2((scores[:, pl.ds(aligned(i * 512, 512), 512)] - best) * scale)
            tot[...] += ((weight[:, 0:128] + weight[:, 128:256])
                         + (weight[:, 256:384] + weight[:, 384:512]))
            acc[...] += dot(weight.astype(BF), kv[pl.ds(r, 512), 128:256])

        total = jnp.sum(tot[...], axis=1, keepdims=True)
        result = (acc[...] / total).astype(BF)
        out[:, h * 128:h * 128 + 128] = result
        sums[4 + h:5 + h, :] = jnp.sum(result.astype(F32), axis=0, keepdims=True)


def call_attend(*args):
    return pl.pallas_call(
        attend,
        out_shape=[jax.ShapeDtypeStruct((256, 512), BF), jax.ShapeDtypeStruct((8, 128), F32)],
        in_specs=[SM, SM, VM, VM, VM],
        out_specs=[VM] * 2,
        scratch_shapes=[pltpu.VMEM((256, 4608), F32), pltpu.VMEM((256, 128), F32),
                        pltpu.VMEM((256, 128), F32), pltpu.VMEM((256, 128), F32)],
        name="attend",
    )(*args)


def exchange_out(
    att, mam, sums, ao, mo, asum, msum,
    buf_y, buf_x, buf_f, send_x, send_f, sa, ra, sm, rm, sc, ry, rx, rf,
):
    X, Y, Z, H, C = coords()
    half = lax.div(Z, 2)
    bar = pltpu.get_barrier_semaphore()
    near = [(o, e) for o in range(4) for e in (0, 1) if o or e]

    def near_id(o, e):
        return {"zl": lax.rem(Z + o, 4), "c": lax.rem(C + e, 2)}

    for o, e in near:
        pl.semaphore_signal(bar, 1, device_id=near_id(o, e), device_id_type=MESH_ID)
    for d in range(1, 4):
        for name, mine in (("X", X), ("Y", Y)):
            pl.semaphore_signal(
                bar, 1, device_id={name: lax.rem(mine + d, 4)}, device_id_type=MESH_ID)
    pl.semaphore_wait(bar, 13)

    def along(name, mine, d, src, buf, recv, first):
        return pltpu.make_async_remote_copy(
            src, buf.at[mine], sc.at[first + d], recv.at[mine],
            device_id={name: lax.rem(mine + d, 4)}, device_id_type=MESH_ID)

    def cols_of(block):
        return pl.ds(aligned(block * 512, 512), 512)

    def mam_copy(o):
        zl = lax.rem(Z + o, 4)
        return pltpu.make_async_remote_copy(
            mam.at[pl.ds(aligned(zl * 128, 128), 128), :], mo.at[:, cols_of(Z)],
            sm.at[o], rm.at[Z], device_id={"zl": zl}, device_id_type=MESH_ID)

    def att_copy(j):
        return pltpu.make_async_remote_copy(
            att.at[j * 128:j * 128 + 128, :], ao.at[:, cols_of(lax.rem(Z, 2))],
            sa.at[j], ra.at[lax.rem(Z, 2)],
            device_id={"zl": 2 * C + j, "c": half}, device_id_type=MESH_ID)

    for d in range(1, 4):
        along("Y", Y, d, sums, buf_y, ry, 0).start()
    for o in (2, 1, 3):
        mam_copy(o).start()
    for j in range(2):
        mine = jnp.logical_and(2 * C + j == Z, half == C)

        @pl.when(jnp.logical_not(mine))
        def _():
            att_copy(j).start()

        @pl.when(mine)
        def _():
            ao[:, cols_of(lax.rem(Z, 2))] = att[j * 128:j * 128 + 128, :]
    buf_y[Y] = sums[...]
    mo[:, cols_of(Z)] = mam[pl.ds(aligned(Z * 128, 128), 128), :]

    for d in range(1, 4):
        n = lax.rem(Y + d, 4)
        landed(buf_y.at[n], ry.at[n])
    send_x[...] = (buf_y[0] + buf_y[1]) + (buf_y[2] + buf_y[3])
    for d in range(1, 4):
        along("X", X, d, send_x, buf_x, rx, 4).start()
    buf_x[X] = send_x[...]
    for d in range(1, 4):
        n = lax.rem(X + d, 4)
        landed(buf_x.at[n], rx.at[n])
    send_f[...] = (buf_x[0] + buf_x[1]) + (buf_x[2] + buf_x[3])
    place = Z * 2 + C

    def last_copy(o, e):
        return pltpu.make_async_remote_copy(
            send_f, buf_f.at[place], sc.at[8 + o * 2 + e], rf.at[place],
            device_id=near_id(o, e), device_id_type=MESH_ID)

    for o, e in near:
        last_copy(o, e).start()
    buf_f[place] = send_f[...]
    for o, e in near:
        n = lax.rem(Z + o, 4) * 2 + lax.rem(C + e, 2)
        landed(buf_f.at[n], rf.at[n])
    for n in range(4):
        msum[n * 4:n * 4 + 4, :] = buf_f[n * 2 + C, 0:4, :]
    for j in range(2):
        first = (2 * C + j) * 2
        asum[j * 4:j * 4 + 4, :] = buf_f[first, 4:8, :] + buf_f[first + 1, 4:8, :]

    for o in range(1, 4):
        n = lax.rem(Z + o, 4)
        landed(mo.at[:, cols_of(n)], rm.at[n])
    for j in range(2):
        @pl.when(jnp.logical_or(2 * C + j != Z, half != C))
        def _():
            landed(ao.at[:, j * 512:j * 512 + 512], ra.at[j])

    for d in range(1, 4):
        along("Y", Y, d, sums, buf_y, ry, 0).wait_send()
        along("X", X, d, send_x, buf_x, rx, 4).wait_send()
        mam_copy(d).wait_send()
    for o, e in near:
        last_copy(o, e).wait_send()
    for j in range(2):
        @pl.when(jnp.logical_or(2 * C + j != Z, half != C))
        def _():
            att_copy(j).wait_send()


def call_exchange_out(*args):
    dma = pltpu.SemaphoreType.DMA
    tile = pltpu.VMEM((8, 128), F32)
    return pl.pallas_call(
        exchange_out,
        out_shape=[jax.ShapeDtypeStruct((128, 1024), BF), jax.ShapeDtypeStruct((128, 2048), BF),
                   jax.ShapeDtypeStruct((8, 128), F32), jax.ShapeDtypeStruct((16, 128), F32)],
        in_specs=[VM] * 3,
        out_specs=[VM] * 4,
        scratch_shapes=[
            pltpu.VMEM((4, 8, 128), F32), pltpu.VMEM((4, 8, 128), F32), pltpu.VMEM((8, 8, 128), F32),
            tile, tile, dma((2,)), dma((2,)), dma((4,)), dma((4,)), dma((16,)),
            dma((4,)), dma((4,)), dma((8,)),
        ],
        compiler_params=pltpu.CompilerParams(collective_id=3, has_side_effects=True),
        name="exchange_out",
    )(*args)


def local(
    queries, keys, values, mamba_x, mamba_b, mamba_c, mamba_dt, conv_x, conv_b, conv_c,
    dt_bias, decay_rate, skip_gain, norm_gain, windows, doc_lengths,
):
    q, kv, x, b, c, dt, tx, tb, tc = call_exchange_in(
        (queries, keys, values, mamba_x, mamba_b, mamba_c, mamba_dt))
    base, inflow, cc, part, decay, send = call_mamba_local(
        doc_lengths, x, b, c, dt, tx, tb, tc, conv_x, conv_b, conv_c,
        dt_bias.reshape(1, 32), decay_rate.reshape(1, 32), skip_gain.reshape(1, 32))
    inc = call_pass_states(send)
    mam, msum = call_mamba_finish(
        base, inflow, cc, part, decay, inc, norm_gain.reshape(1, 2048))
    att, sums = call_attend(windows, doc_lengths, q, kv, msum)
    ao, mo, asum, ms = call_exchange_out(att, mam, sums)
    return ao, mo, asum.reshape(1024), ms.reshape(2048)


def solution(mesh):
    torus = Mesh(mesh.devices.reshape(4, 4, 4, 2, 2), AXES)
    tokens = P(AXES, None)
    tensor = ("zh", "c")
    in_specs = (tokens,) * 7 + (P(None, tensor),) * 3 + (P(tensor),) * 4 + (P(), P())
    out_specs = (P(("X", "Y", "zl"), tensor), P(("X", "Y", "zl"), tensor), P(tensor), P(tensor))
    return jax.shard_map(local, mesh=torus, in_specs=in_specs, out_specs=out_specs, check_vma=False)
```

```python
import math

import jax
import jax.numpy as jnp
from jax import lax
from jax.experimental import pallas as pl
from jax.experimental.pallas import tpu as pltpu
from jax.sharding import Mesh
from jax.sharding import PartitionSpec as P

AXES = ("X", "Y", "zl", "zh", "c")
MESH_ID = pl.DeviceIdType.MESH
BF = jnp.bfloat16
F32 = jnp.float32
HIGH = lax.Precision.HIGHEST
NEG_LARGE = -1e30
EPS_NORM = 1e-05
SUPER = 512
KV_ROWS = 5120
BACK = 4352
VM = pl.BlockSpec(memory_space=pltpu.VMEM)
SM = pl.BlockSpec(memory_space=pltpu.SMEM)
NT = (((1,), (1,)), ((), ()))
TN = (((0,), (0,)), ((), ()))


def coords():
    return tuple(lax.axis_index(a) for a in AXES)


def aligned(v, n):
    return pl.multiple_of(v, n)


def landed(dst, sem):
    pltpu.make_async_copy(dst, dst, sem).wait()


def spread_matrix(rows, cols):
    a = lax.broadcasted_iota(jnp.int32, (rows, cols), 0)
    b = lax.broadcasted_iota(jnp.int32, (rows, cols), 1)
    if rows < cols:
        return (lax.div(b, 64) == a).astype(F32)
    return (lax.div(a, 64) == b).astype(F32)


def dot(a, b, dims=(((1,), (0,)), ((), ())), precision=None):
    return lax.dot_general(a, b, dims, precision=precision, preferred_element_type=F32)


def doc_of(pos, s1, s2):
    one = jnp.where(pos >= s1, 1, 0) + jnp.where(pos >= s2, 1, 0)
    return jnp.where(pos >= 0, one, -1)


def softplus(z):
    return jnp.maximum(z, 0.0) + jnp.log1p(jnp.exp(-jnp.abs(z)))


def layer(
    q, k, v, x, b, c, dt, conv_x, conv_b, conv_c, bias, rate, skip, gain, windows, lens,
    ao, mo, asum, msum,
    qo, kvo, xo, bo, co, dto, txo, tbo, tco, xs, bs, cs,
    base_o, inflow_o, cc_o, part_o, decay_o, send, got, back, inc,
    scores, top, acc, tot, low_o, qs, att, mam, sums,
    buf_y, buf_x, buf_f, send_x, send_f,
    sq, rq, sx, rx, st, rt, sg, rg, sf, rf, s1, r1, s2, r2, sa, ra, sm, rm, sc, ry, rxx, rff,
):
    X, Y, Z, H, C = coords()
    s = X * 4 + Y
    T = H * 2 + C
    u = Z * 4 + T
    zz = H * 4 + Z
    half = lax.div(Z, 2)
    bar = pltpu.get_barrier_semaphore()

    def signal(**where):
        pl.semaphore_signal(bar, 1, device_id=where, device_id_type=MESH_ID)

    def remote(src, dst, ssem, rsem, where):
        return pltpu.make_async_remote_copy(
            src, dst, ssem, rsem, device_id=where, device_id_type=MESH_ID)

    def at(super_index):
        n = lax.rem(super_index + 16, 16)
        return {"X": lax.div(n, 4), "Y": lax.rem(n, 4)}

    def chip(o):
        n = lax.rem(zz + o, 8)
        return lax.div(n, 4), lax.rem(n, 4)

    order8 = (4, 3, 5, 2, 6, 1, 7)
    order16 = [(o, e) for o in order8 for e in (0, 1)] + [(0, 1)]

    for o, e in order16:
        zh, zl = chip(o)
        signal(zl=zl, zh=zh, c=lax.rem(C + e, 2))
    for d in range(1, 16):
        signal(**at(s + d))

    @pl.when(jnp.logical_and(C == 0, s >= 9))
    def _():
        signal(**at(s - 9), c=1)
    signal(**at(s - 1), zl=3, zh=1, c=1)

    kvo[0:128, :] = jnp.zeros((128, 256), BF)
    kvo[4864:5120, :] = jnp.zeros((256, 256), BF)
    expected = 30 + jnp.where(jnp.logical_and(C == 1, s <= 6), 1, 0) + jnp.where(u == 15, 16, 0)
    pl.semaphore_wait(bar, expected)

    srow = lax.rem(Z, 2) * 128 + T * 32
    slot = lax.rem(Z, 2) * 4 + T

    def qkv_parts(o):
        zh, zl = chip(o)
        g = zh * 4 + zl
        krow = BACK + half * 256 + srow
        k_dst = kvo.at[pl.ds(aligned(krow, 32), 32), 0:128]
        v_dst = kvo.at[pl.ds(aligned(krow, 32), 32), 128:256]
        q_dst = qo.at[pl.ds(aligned(srow, 32), 32), :]
        k_src = k.at[:, pl.ds(aligned(g * 128, 128), 128)]
        v_src = v.at[:, pl.ds(aligned(g * 128, 128), 128)]
        q_src = q.at[:, pl.ds(aligned(g * 512, 512), 512)]
        return {"zh": zh, "zl": zl, "c": half}, ((k_src, k_dst), (v_src, v_dst), (q_src, q_dst))

    def qkv_copy(o, i):
        where, parts = qkv_parts(o)
        src, dst = parts[i]
        return remote(src, dst, sq.at[i, o], rq.at[i, slot], where)

    def qkv_start(kinds):
        for o in order8:
            for i in kinds:
                qkv_copy(o, i).start()

        @pl.when(half != C)
        def _():
            for i in kinds:
                qkv_copy(0, i).start()

        @pl.when(half == C)
        def _():
            parts = qkv_parts(0)[1]
            for i in kinds:
                src, dst = parts[i]
                dst[...] = src[...]

    def columns(o, e):
        zh, zl = chip(o)
        cc = lax.rem(C + e, 2)
        tensor = zh * 2 + cc
        xcol = tensor * 2048 + zl * 512
        gcol = (tensor * 2 + lax.div(zl, 2)) * 128
        wide = pl.ds(aligned(xcol, 512), 512)
        thin = pl.ds(aligned(gcol, 128), 128)
        return {"zh": zh, "zl": zl, "c": cc}, wide, thin

    def col_parts(o, e):
        where, wide, thin = columns(o, e)
        rows = pl.ds(aligned(u * 32, 32), 32)
        return where, (
            (dt, dto.at[rows, :]),
            (b.at[:, thin], bo.at[rows, :]),
            (c.at[:, thin], co.at[rows, :]),
            (x.at[:, wide], xo.at[rows, :]),
        )

    def col_copy(o, e, i):
        where, parts = col_parts(o, e)
        src, dst = parts[i]
        return remote(src, dst, sx.at[i, o * 2 + e], rx.at[i, u], where)

    def tail_copy(o, e, i):
        where, wide, thin = columns(o, e)
        src, dst, col = ((x, txo, wide), (b, tbo, thin), (c, tco, thin))[i]
        return remote(src.at[16:32, col], dst, st.at[i, o * 2 + e], rt.at[i], {**at(s + 1), **where})

    qkv_start((0, 1))
    for i in range(4):
        for o, e in order16:
            col_copy(o, e, i).start()
    for i, (src, dst) in enumerate(col_parts(0, 0)[1]):
        dst[...] = src[...]

    @pl.when(u == 15)
    def _():
        for o in range(8):
            for e in (0, 1):
                for i in range(3):
                    tail_copy(o, e, i).start()
    qkv_start((2,))

    def qkv_landed(i):
        for j in range(2):
            for t in range(4):
                row = j * 128 + t * 32
                if i == 2:
                    dst = qo.at[row:row + 32, :]
                else:
                    krow = aligned(BACK + C * 256 + row, 32)
                    dst = kvo.at[pl.ds(krow, 32), i * 128:i * 128 + 128]

                @pl.when(jnp.logical_or(2 * C + j != Z, T != t))
                def _():
                    landed(dst, rq.at[i, j * 4 + t])

    qkv_landed(0)
    qkv_landed(1)

    def half_rows(d):
        return kvo.at[pl.ds(aligned(BACK - SUPER * d + C * 256, 256), 256), :]

    def partner_rows(d):
        return kvo.at[pl.ds(aligned(BACK - SUPER * d + (1 - C) * 256, 256), 256), :]

    def pass_on(d):
        return remote(half_rows(0), half_rows(d), sg.at[d], rg.at[d], at(s + d))

    def pass_last():
        return remote(kvo.at[BACK + 384:BACK + 512, :], kvo.at[128:256, :], sg.at[9], rg.at[9],
                      {**at(s + 9), "c": 0})

    def to_partner(d):
        return remote(half_rows(d), half_rows(d), sf.at[d], rf.at[d], {"c": 1 - C})

    last_out = jnp.logical_and(C == 1, s <= 6)
    for d in range(1, 9):
        @pl.when(s + d < 16)
        def _():
            pass_on(d).start()

    @pl.when(last_out)
    def _():
        pass_last().start()
    to_partner(0).start()

    def forward(d):
        @pl.when(s >= d)
        def _():
            landed(half_rows(d), rg.at[d])
            to_partner(d).start()

    for i in range(4):
        for o, e in order16:
            zs = lax.rem(zz + 8 - o, 8)
            us = lax.rem(zs, 4) * 4 + lax.div(zs, 4) * 2 + lax.rem(C + e, 2)
            dst = (dto, bo, co, xo)[i].at[pl.ds(aligned(us * 32, 32), 32), :]
            landed(dst, rx.at[i, us])
    for i in range(3):
        landed((txo, tbo, tco)[i], rt.at[i])

    st1 = lens[0]
    st2 = lens[0] + lens[1]
    p0 = s * SUPER
    own = (lax.broadcasted_iota(jnp.int32, (8, 32), 1)
           == lax.broadcasted_iota(jnp.int32, (8, 32), 0) + 8 * Z)

    def column(ref):
        return jnp.sum(jnp.where(own, ref[...], 0.0), axis=1, keepdims=True)

    pick32 = (lax.broadcasted_iota(jnp.int32, (32, 8), 0)
              == lax.broadcasted_iota(jnp.int32, (32, 8), 1) + 8 * Z).astype(F32)

    def row(ref):
        return dot(ref[...], pick32, precision=HIGH)

    first_head = T * 32 + Z * 8
    pick = (lax.broadcasted_iota(jnp.int32, (128, 8), 0)
            == lax.broadcasted_iota(jnp.int32, (128, 8), 1) + first_head).astype(BF)
    dcol = softplus(dot(dto[...], pick) + row(bias))
    drow = softplus(dot(pick, dto[...], (((0,), (1,)), ((), ()))) + column(bias))
    lcol = -dcol * row(rate)
    lrow = -drow * column(rate)
    wide = spread_matrix(8, 512)
    tall = spread_matrix(512, 8)
    skip_wide = dot(row(skip), wide, precision=HIGH)

    for src, tail, buf in ((xo, txo, xs), (bo, tbo, bs), (co, tco, cs)):
        buf[0:16, :] = tail[...].astype(F32)
        buf[16:528, :] = src[...].astype(F32)
    taps_x = conv_x[:, pl.ds(aligned(Z * 512, 512), 512)].astype(F32)
    group = pl.ds(aligned(half * 128, 128), 128)
    taps_b = conv_b[:, group].astype(F32)
    taps_c = conv_c[:, group].astype(F32)

    ti = lax.broadcasted_iota(jnp.int32, (128, 128), 0)
    si = lax.broadcasted_iota(jnp.int32, (128, 128), 1)
    lower = (ti >= si).astype(F32)
    upper = (ti <= si).astype(F32)
    state = jnp.zeros((512, 128), F32)
    decay = jnp.ones((8, 128), F32)
    for n in range(4):
        part_o[n] = state
        decay_o[n] = decay
        pb = p0 + n * 128
        rows = slice(n * 128, n * 128 + 128)
        pcol = pb + lax.broadcasted_iota(jnp.int32, (128, 1), 0)
        prow = pb + lax.broadcasted_iota(jnp.int32, (1, 128), 1)
        start = jnp.where(pcol >= st2, st2, jnp.where(pcol >= st1, st1, 0))
        keep = [pcol - j >= start for j in range(4)]

        def conv(buf, taps):
            total = None
            for j in range(4):
                lo = 16 + n * 128 - j
                term = taps[j:j + 1, :] * buf[lo:lo + 128, :]
                if j:
                    term = jnp.where(keep[j], term, 0.0)
                total = term if total is None else total + term
            return (total / (1.0 + jnp.exp(-total))).astype(BF)

        xc = conv(xs, taps_x)
        bc = conv(bs, taps_b)
        cc = conv(cs, taps_c)
        cc_o[rows, :] = cc
        ccol = dot(lower, lcol[rows, :], precision=HIGH)
        crow = dot(lrow[:, rows], upper, precision=HIGH)
        doc_c = doc_of(pcol, st1, st2)
        doc_r = doc_of(prow, st1, st2)
        allowed = jnp.logical_and(ti >= si, doc_c == doc_r)
        cross = jnp.where(allowed, dot(cc, bc, NT), 0.0)
        xf = xc.astype(F32)
        for pair in range(4):
            mixes = []
            for h in (2 * pair, 2 * pair + 1):
                gap = ccol[:, h:h + 1] - crow[h:h + 1, :]
                seg = jnp.exp(jnp.minimum(gap, 0.0))
                mixes.append((seg * cross * drow[h:h + 1, rows]).astype(BF))
            xp = xc[:, pair * 128:pair * 128 + 128]
            zero = jnp.zeros_like(xp)
            both = jnp.concatenate(
                [jnp.where(si < 64, xp, zero), jnp.where(si < 64, zero, xp)], axis=0)
            intra = dot(jnp.concatenate(mixes, axis=1), both)
            cols = slice(pair * 128, pair * 128 + 128)
            base_o[rows, cols] = intra + skip_wide[:, cols] * xf[:, cols]
        doc_e = doc_of(pb + 127, st1, st2)
        doc_p = doc_of(pb - 1, st1, st2)
        to_end = jnp.where(doc_c == doc_e, jnp.exp(ccol[127:128, :] - ccol), 0.0) * dcol[rows, :]
        weighted = (dot(to_end, wide, precision=HIGH) * xf).astype(BF)
        factor = jnp.where(doc_p == doc_e, jnp.exp(crow[:, 127:128]), 0.0)
        factor = jnp.broadcast_to(factor, (8, 128))
        inflow_o[rows, :] = jnp.where(doc_c == doc_p, jnp.exp(ccol), 0.0)
        state = dot(tall, factor, precision=HIGH) * state + dot(weighted, bc, TN)
        decay = factor * decay
        forward(2 * n + 1)
        forward(2 * n + 2)
    for j in range(16):
        send[j, 0:32, :] = state[j * 32:j * 32 + 32, :]
        send[j, 32:40, :] = jnp.broadcast_to(decay[j // 2:j // 2 + 1, :], (8, 128))

    def peer(d):
        n = lax.rem(s + d, 16)
        return n, {"X": lax.div(n, 4), "Y": lax.rem(n, 4)}

    def there(d):
        n, where = peer(d)
        return remote(send.at[n], got.at[s], s1.at[d], r1.at[s], where)

    inc_rows = pl.ds(aligned(s * 32, 32), 32)

    def again(d):
        n, where = peer(d)
        return remote(back.at[n], inc.at[inc_rows, :], s2.at[d], r2.at[s], where)

    qkv_landed(2)
    t0 = s * SUPER + C * 256
    first = s * SUPER - BACK
    tcol = t0 + lax.broadcasted_iota(jnp.int32, (256, 1), 0)
    start_col = jnp.where(tcol >= st2, st2, jnp.where(tcol >= st1, st1, 0))
    for h in range(4):
        w = windows[zz * 4 + h]
        low = jnp.maximum(tcol - w + 1, start_col)
        low_o[h * 256:h * 256 + 256, :] = jnp.broadcast_to(low, (256, 128))
        qs[h * 256:h * 256 + 256, :] = qo[:, h * 128:h * 128 + 128]
    for d in range(1, 16):
        there(d).start()
    got[s] = send[s]
    top[...] = jnp.full((1024, 128), NEG_LARGE, F32)
    acc[...] = jnp.zeros((1024, 128), F32)
    tot[...] = jnp.zeros((1024, 128), F32)

    @pl.when(jnp.logical_and(C == 0, s >= 9))
    def _():
        landed(kvo.at[128:256, :], rg.at[9])
    landed(partner_rows(0), rf.at[0])
    for d in range(1, 9):
        @pl.when(s >= d)
        def _():
            landed(partner_rows(d), rf.at[d])

    end_row = BACK + C * 256 + 256
    c0 = jnp.maximum(C, 17 - 2 * s)
    count = lax.div(end_row - c0 * 256 + 511, 512)
    lane = lax.broadcasted_iota(jnp.int32, (1, 128), 1)
    trow = t0 + lax.broadcasted_iota(jnp.int32, (256, 128), 0)

    def score_chunk(i, causal):
        r = aligned(c0 * 256 + i * 512, 256)
        keys = kvo[pl.ds(r, 512), 0:128]
        score = dot(qs[...], keys, NT)
        best = None
        for j in range(4):
            part = score[:, j * 128:j * 128 + 128]
            kpos = first + r + j * 128 + lane
            ok = kpos >= low_o[...]
            if causal:
                ok = jnp.logical_and(ok, jnp.concatenate([kpos <= trow] * 4, axis=0))
            part = jnp.where(ok, part, NEG_LARGE)
            scores[:, pl.ds(aligned(i * 512 + j * 128, 128), 128)] = part
            best = part if best is None else jnp.maximum(best, part)
        top[...] = jnp.maximum(top[...], best)

    @pl.loop(0, count - 1)
    def _(i):
        score_chunk(i, False)
    score_chunk(count - 1, True)

    for d in range(1, 16):
        n, _ = peer(16 - d)
        landed(got.at[n], r1.at[n])
    value = jnp.zeros((4, 8, 128), F32)
    for n in range(16):
        back[n] = value.reshape(32, 128).astype(BF)
        value = got[n, 32:40, :][None] * value + got[n, 0:32, :].reshape(4, 8, 128)
    inc[inc_rows, :] = back[s]
    top[...] = jnp.broadcast_to(jnp.max(top[...], axis=1, keepdims=True), (1024, 128))
    for d in range(1, 16):
        again(d).start()

    scale = math.log2(math.e) / math.sqrt(128)

    @pl.loop(0, count)
    def _(i):
        r = aligned(c0 * 256 + i * 512, 256)
        best = top[...]
        weights = [
            jnp.exp2((scores[:, pl.ds(aligned(i * 512 + j * 128, 128), 128)] - best) * scale)
            for j in range(4)
        ]
        tot[...] += (weights[0] + weights[1]) + (weights[2] + weights[3])
        weight = jnp.concatenate([part.astype(BF) for part in weights], axis=1)
        acc[...] += dot(weight, kvo[pl.ds(r, 512), 128:256])

    for h in range(4):
        rows = slice(h * 256, h * 256 + 256)
        total = jnp.sum(tot[rows, :], axis=1, keepdims=True)
        result = (acc[rows, :] / total).astype(BF)
        att[:, h * 128:h * 128 + 128] = result
        sums[4 + h:5 + h, :] = jnp.sum(result.astype(F32), axis=0, keepdims=True)

    def cols_of(block):
        return pl.ds(aligned(block * 512, 512), 512)

    def mam_copy(n):
        return remote(mam.at[pl.ds(aligned(n * 128, 128), 128), :], mo.at[:, cols_of(Z)],
                      sm.at[n], rm.at[Z], {"zl": n})

    def att_copy(j):
        return remote(att.at[j * 128:j * 128 + 128, :], ao.at[:, cols_of(lax.rem(Z, 2))],
                      sa.at[j], ra.at[lax.rem(Z, 2)], {"zl": 2 * C + j, "c": half})

    for d in range(1, 16):
        n, _ = peer(16 - d)
        landed(inc.at[pl.ds(aligned(n * 32, 32), 32), :], r2.at[n])
    for j in range(2):
        mine = jnp.logical_and(2 * C + j == Z, half == C)

        @pl.when(jnp.logical_not(mine))
        def _():
            att_copy(j).start()

        @pl.when(mine)
        def _():
            ao[:, cols_of(lax.rem(Z, 2))] = att[j * 128:j * 128 + 128, :]

    gain_row = gain[:, pl.ds(aligned(Z * 512, 512), 512)]
    average = jnp.where(lax.div(ti, 64) == lax.div(si, 64), 1.0 / 64, 0.0).astype(F32)
    entering = inc[...].astype(F32)
    total = jnp.zeros((1, 512), F32)
    for o in range(4):
        n = lax.rem(Z + 1 + o, 4)
        rows = pl.ds(aligned(n * 128, 128), 128)
        state = (dot(tall, decay_o[n], precision=HIGH) * entering + part_o[n]).astype(BF)
        flow = dot(inflow_o[rows, :], wide, precision=HIGH)
        full = base_o[rows, :] + dot(cc_o[rows, :], state, NT) * flow
        for pair in range(4):
            cols = slice(pair * 128, pair * 128 + 128)
            f = full[:, cols]
            mean = dot(f * f, average, precision=HIGH)
            result = (f * lax.rsqrt(mean + EPS_NORM) * gain_row[:, cols]).astype(BF)
            mam[rows, cols] = result
            sums_part = jnp.sum(result.astype(F32), axis=0, keepdims=True)
            if o == 0:
                sums[pair:pair + 1, :] = sums_part
            else:
                sums[pair:pair + 1, :] += sums_part
        if o:
            mam_copy(lax.rem(Z + o, 4)).start()
    mo[:, cols_of(Z)] = mam[pl.ds(aligned(Z * 128, 128), 128), :]

    def along(name, mine, d, src, buf, recv, base):
        return remote(src, buf.at[mine], sc.at[base + d], recv.at[mine], {name: lax.rem(mine + d, 4)})

    near = [(o, e) for o in range(4) for e in (0, 1) if o or e]
    for d in range(1, 4):
        along("Y", Y, d, sums, buf_y, ry, 0).start()
    buf_y[Y] = sums[...]
    for d in range(1, 4):
        n = lax.rem(Y + d, 4)
        landed(buf_y.at[n], ry.at[n])
    send_x[...] = (buf_y[0] + buf_y[1]) + (buf_y[2] + buf_y[3])
    buf_x[X] = send_x[...]
    for d in range(1, 4):
        along("X", X, d, send_x, buf_x, rxx, 4).start()
    for d in range(1, 4):
        n = lax.rem(X + d, 4)
        landed(buf_x.at[n], rxx.at[n])
    place = Z * 2 + C
    send_f[...] = (buf_x[0] + buf_x[1]) + (buf_x[2] + buf_x[3])
    buf_f[place] = send_f[...]

    def last_copy(o, e):
        return remote(send_f, buf_f.at[place], sc.at[8 + o * 2 + e], rff.at[place],
                      {"zl": lax.rem(Z + o, 4), "c": lax.rem(C + e, 2)})

    for o, e in near:
        last_copy(o, e).start()

    for i in range(3):
        for o in order8:
            qkv_copy(o, i).wait_send()

        @pl.when(half != C)
        def _():
            qkv_copy(0, i).wait_send()
    for i in range(4):
        for o, e in order16:
            col_copy(o, e, i).wait_send()

    @pl.when(u == 15)
    def _():
        for o in range(8):
            for e in (0, 1):
                for i in range(3):
                    tail_copy(o, e, i).wait_send()
    to_partner(0).wait_send()
    for d in range(1, 9):
        @pl.when(s + d < 16)
        def _():
            pass_on(d).wait_send()

        @pl.when(s >= d)
        def _():
            to_partner(d).wait_send()

    @pl.when(last_out)
    def _():
        pass_last().wait_send()
    for d in range(1, 16):
        there(d).wait_send()
        again(d).wait_send()

    for o, e in near:
        n = lax.rem(Z + o, 4) * 2 + lax.rem(C + e, 2)
        landed(buf_f.at[n], rff.at[n])
    for n in range(4):
        msum[n * 4:n * 4 + 4, :] = buf_f[n * 2 + C, 0:4, :]
    for j in range(2):
        spot = (2 * C + j) * 2
        asum[j * 4:j * 4 + 4, :] = buf_f[spot, 4:8, :] + buf_f[spot + 1, 4:8, :]
    for j in range(2):
        @pl.when(jnp.logical_or(2 * C + j != Z, half != C))
        def _():
            landed(ao.at[:, j * 512:j * 512 + 512], ra.at[j])
            att_copy(j).wait_send()
    for d in range(1, 4):
        n = lax.rem(Z + d, 4)
        landed(mo.at[:, cols_of(n)], rm.at[n])
        mam_copy(n).wait_send()
        along("Y", Y, d, sums, buf_y, ry, 0).wait_send()
        along("X", X, d, send_x, buf_x, rxx, 4).wait_send()
    for o, e in near:
        last_copy(o, e).wait_send()


def call_layer(*args):
    dma = pltpu.SemaphoreType.DMA
    shapes = (
        ((256, 512), BF), ((KV_ROWS, 256), BF), ((512, 512), BF), ((512, 128), BF),
        ((512, 128), BF), ((512, 128), BF), ((16, 512), BF), ((16, 128), BF), ((16, 128), BF),
        ((528, 512), F32), ((528, 128), F32), ((528, 128), F32),
        ((512, 512), F32), ((512, 8), F32), ((512, 128), BF), ((4, 512, 128), F32),
        ((4, 8, 128), F32), ((16, 40, 128), F32), ((16, 40, 128), F32), ((16, 32, 128), BF),
        ((512, 128), BF),
        ((1024, 4608), F32), ((1024, 128), F32), ((1024, 128), F32), ((1024, 128), F32),
        ((1024, 128), jnp.int32), ((1024, 128), BF), ((256, 512), BF), ((512, 512), BF),
        ((8, 128), F32),
        ((4, 8, 128), F32), ((4, 8, 128), F32), ((8, 8, 128), F32), ((8, 128), F32),
        ((8, 128), F32),
    )
    sems = ((3, 8), (3, 8), (4, 16), (4, 16), (3, 16), (3,), (10,), (10,), (9,), (9,),
            (16,), (16,), (16,), (16,), (2,), (2,), (4,), (4,), (16,), (4,), (4,), (8,))
    outs = (((128, 1024), BF), ((128, 2048), BF), ((8, 128), F32), ((16, 128), F32))
    return pl.pallas_call(
        layer,
        out_shape=[pltpu.VMEM(n, t) for n, t in outs],
        in_specs=[VM] * 14 + [SM] * 2,
        out_specs=[VM] * 4,
        scratch_shapes=[pltpu.VMEM(n, t) for n, t in shapes] + [dma(n) for n in sems],
        compiler_params=pltpu.CompilerParams(
            collective_id=1, has_side_effects=True, vmem_limit_bytes=56 << 20),
        name="layer",
    )(*args)


def emit(a, b, c, d, ao, bo, co, do, sem):
    copies = [pltpu.make_async_copy(src, dst, sem.at[i])
              for i, (src, dst) in enumerate(((a, ao), (b, bo), (c, co), (d, do)))]
    for copy in copies:
        copy.start()
    for copy in copies:
        copy.wait()


def call_emit(*args):
    return pl.pallas_call(
        emit,
        out_shape=[jax.ShapeDtypeStruct(a.shape, a.dtype) for a in args],
        in_specs=[VM] * 4,
        out_specs=[pl.BlockSpec(memory_space=pl.ANY)] * 4,
        scratch_shapes=[pltpu.SemaphoreType.DMA((4,))],
        name="emit",
    )(*args)


def local(
    queries, keys, values, mamba_x, mamba_b, mamba_c, mamba_dt, conv_x, conv_b, conv_c,
    dt_bias, decay_rate, skip_gain, norm_gain, windows, doc_lengths,
):
    results = call_layer(
        queries, keys, values, mamba_x, mamba_b, mamba_c, mamba_dt, conv_x, conv_b, conv_c,
        dt_bias.reshape(1, 32), decay_rate.reshape(1, 32), skip_gain.reshape(1, 32),
        norm_gain.reshape(1, 2048), windows, doc_lengths)
    ao, mo, asum, msum = results
    return ao, mo, asum.reshape(1024), msum.reshape(2048)


def solution(mesh):
    torus = Mesh(mesh.devices.reshape(4, 4, 4, 2, 2), AXES)
    tokens = P(AXES, None)
    tensor = ("zh", "c")
    in_specs = (tokens,) * 7 + (P(None, tensor),) * 3 + (P(tensor),) * 4 + (P(), P())
    out_specs = (P(("X", "Y", "zl"), tensor), P(("X", "Y", "zl"), tensor), P(tensor), P(tensor))
    return jax.shard_map(local, mesh=torus, in_specs=in_specs, out_specs=out_specs, check_vma=False)
```
